32 devices in a mesh: dp: 4 (over z), ctx: 4 (over y, core), wshard: 2 (over x).
Axes of the slice: x: 2, y: 2, z: 4, core: 2. Of those that a mesh axis runs over, the one named last changes fastest.
Arguments:
- layer_input: bfloat16 [8, 2048, 1088], P(('dp', 'wshard'), 'ctx'), may hold values from -6 to 6
- ln1_gain: bfloat16 [1088], P('wshard'), may hold values from 0.25 to 1.75
- ln1_bias: bfloat16 [1088], P('wshard'), may hold values from -4 to 4
- w_qkv: bfloat16 [1088, 3264], P('wshard'), may hold values from -1 to 1
- q_bias: bfloat16 [1088], P('wshard'), may hold values from -6 to 6
- v_bias: bfloat16 [1088], P('wshard'), may hold values from -6 to 6
- w_out: bfloat16 [1088, 1088], P('wshard'), may hold values from -0.75 to 0.75
- out_bias: bfloat16 [1088], P('wshard'), may hold values from -4 to 4
- ln2_gain: bfloat16 [1088], P('wshard'), may hold values from 0.25 to 1.75
- ln2_bias: bfloat16 [1088], P('wshard'), may hold values from -4 to 4
- w_up: bfloat16 [1088, 4352], P('wshard'), may hold values from -0.1875 to 0.1875
- up_bias: bfloat16 [4352], P('wshard'), may hold values from -4 to 4
- w_down: bfloat16 [4352, 1088], P('wshard'), may hold values from -0.09375 to 0.09375
- down_bias: bfloat16 [1088], P('wshard'), may hold values from -6 to 6
- cotangent: bfloat16 [8, 2048, 1088], P(('dp', 'wshard'), 'ctx'), may hold values from -6 to 6
Outputs:
- layer_output: bfloat16 [8, 2048, 1088], P(('dp', 'wshard'), 'ctx')
- input_grad: bfloat16 [8, 2048, 1088], P(('dp', 'wshard'), 'ctx')
- ln1_gain_grad: float32 [1088], P('wshard')
- ln1_bias_grad: float32 [1088], P('wshard')
- w_qkv_grad: float32 [1088, 3264], P('wshard')
- q_bias_grad: float32 [1088], P('wshard')
- v_bias_grad: float32 [1088], P('wshard')
- w_out_grad: float32 [1088, 1088], P('wshard')
- out_bias_grad: float32 [1088], P('wshard')
- ln2_gain_grad: float32 [1088], P('wshard')
- ln2_bias_grad: float32 [1088], P('wshard')
- w_up_grad: float32 [1088, 4352], P('wshard')
- up_bias_grad: float32 [4352], P('wshard')
- w_down_grad: float32 [4352, 1088], P('wshard')
- down_bias_grad: float32 [1088], P('wshard')
The draws below stay inside these ranges and needn't reach their ends.
All inputs are finite; a program needn't handle non-finite values.
Results may differ from the reference program's by a relative error of at most 0.019.
Values may be sent and summed in bfloat16 or wider, within the bound.
A program may use at most 320 MiB of HBM per device.

```python
import jax
import jax.numpy as jnp
from jax import lax

D = 1088
H = 17
HD = 64
FF = 4352
SEQ_LEN = 2048
SEQS = 8


def draw_w_qkv(key, part):
    first = jax.random.fold_in(key, 0)
    base = jax.random.truncated_normal(first, -4.0, 4.0, (D, 3 * D), jnp.float32) * D ** (-0.5)
    return jnp.clip(base, -1.0, 1.0).astype(jnp.bfloat16)


def block_scale(own_key, extent, cuts, smallest, top_value):
    loudness = 1.0
    for axis_at, shards_of in cuts:
        heights = jax.random.uniform(jax.random.fold_in(jax.random.fold_in(own_key, 6), axis_at), (shards_of,), jnp.float32, smallest / len(cuts), top_value / len(cuts))
        loudness = loudness * jnp.repeat(jnp.exp(heights), extent[axis_at] // shards_of).reshape((-1,) + (1,) * (len(extent) - 1 - axis_at))
    return loudness


def noise(key, dims, scale, reach, shards=(), kind=jnp.bfloat16):
    drawn = jax.random.normal(key, dims, jnp.float32) * scale
    if len(shards) > 0:
        drawn = block_scale(key, dims, shards, -0.22, 0.18) * drawn
    return jnp.clip(drawn, min=-reach, max=reach).astype(kind)


def setup_inputs(seed: int = 0) -> dict:
    splits = jax.random.split(jax.random.key(seed), 16)
    return {
        "layer_input": noise(splits[0], (SEQS, SEQ_LEN, D), 1.0, 6.0, ((0, 8), (1, 4))),
        "ln1_gain": jnp.clip(1.0 + 0.15 * jax.random.normal(splits[1], (D,), jnp.float32), 0.25, 1.75).astype(jnp.bfloat16),
        "ln1_bias": noise(splits[2], (D,), 0.3, 4.0, ((0, 2),)),
        "w_qkv": draw_w_qkv(jax.random.fold_in(splits[15], 71), 0),
        "q_bias": noise(splits[4], (D,), 0.5, 6.0, ((0, 2),)),
        "v_bias": noise(splits[5], (D,), 0.5, 6.0, ((0, 2),)),
        "w_out": noise(splits[6], (D, D), (D // 16) ** -0.5, 0.75, ((0, 2),)),
        "out_bias": noise(splits[7], (D,), 0.3, 4.0, ((0, 2),)),
        "ln2_gain": jnp.clip(1.0 + 0.15 * jax.random.normal(splits[8], (D,), jnp.float32), 0.25, 1.75).astype(jnp.bfloat16),
        "ln2_bias": noise(splits[9], (D,), 0.3, 4.0, ((0, 2),)),
        "w_up": noise(splits[10], (D, FF), D ** -0.5, 0.1875, ((0, 2),)),
        "up_bias": noise(splits[11], (FF,), 0.3, 4.0, ((0, 2),)),
        "w_down": noise(splits[12], (FF, D), FF ** -0.5, 0.09375, ((0, 2),)),
        "down_bias": noise(splits[13], (D,), 0.5, 6.0, ((0, 2),)),
        "cotangent": noise(splits[14], (SEQS, SEQ_LEN, D), 1.0, 6.0, ((0, 8), (1, 4))),
    }


@jax.custom_vjp
def low(v):
    return lax.optimization_barrier(v.astype(jnp.bfloat16)).astype(jnp.float32)

@jax.custom_vjp
def low_back(v):
    return v

def low_keep(v):
    return (low(v), None)

def low_pass(kept, grad):
    return (grad,)

def back_keep(v):
    return (v, None)

def back_low(kept, grad):
    return (low(grad),)
low.defvjp(low_keep, low_pass)
low_back.defvjp(back_keep, back_low)

def layer_norm(values, gain, shift):
    mean = lax.optimization_barrier(jnp.mean(values, axis=-1, keepdims=True))
    centred = values - mean
    variance = lax.optimization_barrier(jnp.mean(centred * centred, axis=-1, keepdims=True))
    return centred * lax.rsqrt(variance + 1e-05) * gain + shift

def matmul(left, right):
    return jnp.dot(left, right, precision=lax.Precision.HIGHEST, preferred_element_type=jnp.float32)

def layer(params, seq):
    gain1, shift1, mat_qkv, bias_q, bias_v, mat_out, bias_out, gain2, shift2, mat_up, bias_up, mat_down, bias_down = params
    span = seq.shape[0]
    normed1 = low(layer_norm(seq, gain1, shift1))
    mixed = matmul(normed1, mat_qkv)
    queries = low(low_back(mixed[:, :D] + bias_q)).reshape(span, H, HD)
    keys = low(low_back(mixed[:, D:2 * D])).reshape(span, H, HD)
    values = low(low_back(mixed[:, 2 * D:] + bias_v)).reshape(span, H, HD)
    scores = low_back(jnp.einsum('qhd,khd->hqk', queries, keys, precision=lax.Precision.HIGHEST) * HD ** (-0.5))
    position = jnp.arange(span, dtype=jnp.int32)
    allowed = position[None, :] <= position[:, None]
    scores = jnp.where(allowed[None, :, :], scores, -1e+30)
    best = lax.optimization_barrier(jnp.max(scores, axis=-1, keepdims=True))
    weights = jnp.exp(scores - best)
    probs = low(weights / lax.optimization_barrier(jnp.sum(weights, axis=-1, keepdims=True)))
    attention = jnp.einsum('hqk,khd->qhd', probs, values, precision=lax.Precision.HIGHEST).reshape(span, D)
    attn_low = low(low_back(attention))
    resid = seq + low_back(matmul(attn_low, mat_out) + bias_out)
    normed2 = low(layer_norm(resid, gain2, shift2))
    upper = low_back(matmul(normed2, mat_up) + bias_up)
    acts = low(jax.nn.gelu(upper, approximate=False))
    return resid + matmul(acts, mat_down) + bias_down

def reference(layer_input, ln1_gain, ln1_bias, w_qkv, q_bias, v_bias, w_out, out_bias, ln2_gain, ln2_bias, w_up, up_bias, w_down, down_bias, cotangent):
    params = tuple((item.astype(jnp.float32) for item in (ln1_gain, ln1_bias, w_qkv, q_bias, v_bias, w_out, out_bias, ln2_gain, ln2_bias, w_up, up_bias, w_down, down_bias)))
    inputs = layer_input.astype(jnp.float32)

    def forward(weights, data):

        def step(carry, seq):
            return (carry, jax.checkpoint(layer)(weights, seq))
        _, result = lax.scan(step, jnp.zeros((), jnp.float32), data)
        return result
    result, pull = jax.vjp(forward, params, inputs)
    grads, input_grad = pull(cotangent.astype(jnp.float32))
    return (result.astype(jnp.bfloat16), input_grad.astype(jnp.bfloat16), grads[0], grads[1], grads[2], grads[3], grads[4], grads[5], grads[6], grads[7], grads[8], grads[9], grads[10], grads[11], grads[12])
```

```python
import jax
import jax.numpy as jnp
from jax import lax
from jax.sharding import PartitionSpec as P

H = 17
F32 = jnp.float32
BF16 = jnp.bfloat16
GRID = ("dp", "ctx")


def layer_norm(values, gain, shift):
    mean = jnp.mean(values, axis=-1, keepdims=True)
    centred = values - mean
    variance = jnp.mean(centred * centred, axis=-1, keepdims=True)
    return centred * lax.rsqrt(variance + 1e-05) * gain + shift


def exact_gelu(values):
    return jax.nn.gelu(values, approximate=False)


def pick(array, index, axis=0):
    return lax.dynamic_index_in_dim(array, index, axis, keepdims=False)


def ordered(first_mine, mine, other):
    return jnp.stack(
        [jnp.where(first_mine, mine, other), jnp.where(first_mine, other, mine)], axis=0
    )


class Links:
    def __init__(self, sizes):
        self.ndp, self.nctx, self.nw = sizes["dp"], sizes["ctx"], sizes["wshard"]
        self.high = self.nctx // 4
        self.rest = self.ndp * self.high
        ctx = lax.axis_index("ctx")
        self.ctx = ctx
        self.side = lax.axis_index("wshard")
        self.core = ctx % 2
        self.row = (ctx // 2) % 2
        self.place = lax.axis_index("dp") * self.high + ctx // 4

    def across(self, array):
        return lax.ppermute(array, "wshard", [(0, 1), (1, 0)])

    def flip(self, array, bit):
        return lax.ppermute(array, "ctx", [(i, i ^ bit) for i in range(self.nctx)])

    def other_core(self, array):
        return self.flip(array, 1)

    def other_row(self, array):
        return self.flip(array, 2)

    def shifted(self, array, step):
        pairs = []
        for place in range(self.rest):
            target = (place + step) % self.rest
            for low in range(4):
                def flat(p):
                    return (p // self.high) * self.nctx + (p % self.high) * 4 + low
                pairs.append((flat(place), flat(target)))
        return lax.ppermute(array, GRID, pairs)


def other_half(links, own):
    rows, cols = own.shape
    parts = own.reshape(2, rows // 2, cols)
    mine = links.across(pick(parts, links.core))
    return ordered(links.core == 0, mine, links.other_core(mine)).reshape(rows, cols)


def window(tiles, count):
    size = -(-tiles // count)
    while count > 1 and ((tiles - size) % (count - 1) != 0 or (tiles - size) // (count - 1) > size):
        size += 1
    return size, ((tiles - size) // (count - 1) if count > 1 else 0)


def total(pieces):
    result = pieces[0].astype(F32)
    for piece in pieces[1:]:
        result = result + piece.astype(F32)
    return result


def reduce_rows(links, grad):
    rows, cols = grad.shape
    tiles = rows // 64
    view = grad.reshape(2, 2, 2, tiles, 8, cols)
    got = links.other_core(pick(view, 1 - links.core, 1))
    have = [pick(view, links.core, 1), got]
    sent = total([pick(item, 1 - links.side) for item in have]).astype(BF16)
    have = [pick(item, links.side) for item in have] + [links.across(sent)]
    sent = total([pick(item, 1 - links.row) for item in have]).astype(BF16)
    have = [pick(item, links.row) for item in have] + [links.other_row(sent)]
    mixed = total(have).astype(BF16)
    size, step = window(tiles, links.rest)

    def slot(index):
        return lax.dynamic_slice_in_dim(mixed, (index % links.rest) * step, size, 0)

    final = [slot(links.place)]
    for shift in range(1, links.rest):
        final.append(links.shifted(slot(links.place + shift), shift))
    done = total(final).astype(BF16)
    whole = jnp.zeros((tiles, 8, cols), BF16)
    whole = lax.dynamic_update_slice_in_dim(whole, done, links.place * step, 0)
    for shift in range(1, links.rest):
        came = (links.place - shift + links.rest) % links.rest
        whole = lax.dynamic_update_slice_in_dim(whole, links.shifted(done, shift), came * step, 0)
    both = ordered(links.row == 0, whole, links.other_row(whole))
    full = ordered(links.core == 0, both, links.other_core(both))
    return full.reshape(rows // 2, cols).astype(F32)


def gather_context(links, own):
    blocks = ordered(links.row == 0, own, links.other_row(own))[:, None]
    for bit in range(2, links.nctx.bit_length() - 1):
        low = (links.ctx // (1 << bit)) % 2 == 0
        blocks = ordered(low, blocks, links.flip(blocks, 1 << bit)).reshape(
            (-1,) + blocks.shape[1:]
        )
    got = links.other_core(blocks)
    first = jnp.where(links.core == 0, blocks, got)
    second = jnp.where(links.core == 0, got, blocks)
    return jnp.concatenate([first, second], axis=1).reshape((links.nctx,) + own.shape)


def grad_block(queries, douts, keys, values, start, query_pos, lse, delta, scale):
    scores = jnp.einsum("qhd,khd->hqk", queries, keys, preferred_element_type=F32) * scale
    key_pos = start + jnp.arange(keys.shape[0], dtype=jnp.int32)
    allowed = key_pos[None, :] <= query_pos[:, None]
    probs = jnp.where(allowed[None], jnp.exp(scores - lse[..., None]), 0.0)
    dprobs = jnp.einsum("qhd,khd->hqk", douts, values, preferred_element_type=F32)
    dscores = (probs * (dprobs - delta[..., None])).astype(BF16)
    dq = jnp.einsum("hqk,khd->qhd", dscores, keys, preferred_element_type=F32) * scale
    dv = jnp.einsum("hqk,qhd->khd", probs.astype(BF16), douts, preferred_element_type=F32)
    dk = jnp.einsum("hqk,qhd->khd", dscores, queries, preferred_element_type=F32) * scale
    return dq, dk, dv


def shards(
    sizes,
    layer_input,
    ln1_gain,
    ln1_bias,
    w_qkv,
    q_bias,
    v_bias,
    w_out,
    out_bias,
    ln2_gain,
    ln2_bias,
    w_up,
    up_bias,
    w_down,
    down_bias,
    cotangent,
):
    links = Links(sizes)
    seqs, blk, width = layer_input.shape
    half = width // 2
    ff = up_bias.shape[0] * 2
    head_dim = width // H
    scale = head_dim ** (-0.5)
    side = links.side

    small = [ln1_gain, ln1_bias, q_bias, v_bias, out_bias, ln2_gain, ln2_bias, down_bias]
    packed = jnp.stack(small, axis=0)
    packed_other = links.across(packed)
    vectors = jnp.where(
        side == 0,
        jnp.concatenate([packed, packed_other], axis=1),
        jnp.concatenate([packed_other, packed], axis=1),
    ).astype(F32)
    gain1, shift1, bias_q, bias_v, bias_out, gain2, shift2, bias_down = (
        vectors[i] for i in range(8)
    )
    bias_up = ordered(side == 0, up_bias, links.across(up_bias)).reshape(ff).astype(F32)

    def whole(own):
        return ordered(side == 0, own, other_half(links, own)).reshape(2 * own.shape[0], own.shape[1])

    mat_qkv = whole(w_qkv)
    mat_out = whole(w_out)
    mat_up = whole(w_up)
    mat_down = whole(w_down)

    span = seqs * links.nctx * blk
    every = gather_context(links, layer_input.reshape(seqs * blk, width)).reshape(span, width)
    rows = layer_input.reshape(seqs * blk, width).astype(F32)
    here = links.ctx
    query_pos = here * blk + jnp.arange(blk, dtype=jnp.int32)
    normed1, ln1_pull = jax.vjp(layer_norm, rows, gain1, shift1)
    normed1_low = normed1.astype(BF16)
    normed_all = layer_norm(every.astype(F32), gain1, shift1).astype(BF16)
    queries = (
        jnp.dot(normed1_low, mat_qkv[:, :width], preferred_element_type=F32) + bias_q
    ).astype(BF16)
    key_values = jnp.dot(normed_all, mat_qkv[:, width:], preferred_element_type=F32)
    keys = key_values[:, :width].astype(BF16)
    values = (key_values[:, width:] + bias_v).astype(BF16)
    queries4 = queries.reshape(blk, H, head_dim)
    keys4 = keys.reshape(span, H, head_dim)
    values4 = values.reshape(span, H, head_dim)
    scores = jnp.einsum("qhd,khd->hqk", queries4, keys4, preferred_element_type=F32) * scale
    allowed = jnp.arange(span, dtype=jnp.int32)[None, :] <= query_pos[:, None]
    scores = jnp.where(allowed[None], scores, -1e30)
    best = jnp.max(scores, axis=-1)
    weights = jnp.exp(scores - best[..., None])
    norm = jnp.sum(weights, axis=-1)
    accum = jnp.einsum("hqk,khd->hqd", weights.astype(BF16), values4, preferred_element_type=F32)
    attention4 = jnp.transpose(accum / norm[..., None], (1, 0, 2))
    lse = best + jnp.log(norm)
    attn_low = attention4.reshape(blk, width).astype(BF16)
    resid = rows + jnp.dot(attn_low, mat_out, preferred_element_type=F32) + bias_out
    normed2, ln2_pull = jax.vjp(layer_norm, resid, gain2, shift2)
    normed2_low = normed2.astype(BF16)
    upper = jnp.dot(normed2_low, mat_up, preferred_element_type=F32) + bias_up
    acts, gelu_pull = jax.vjp(exact_gelu, upper)
    acts_low = acts.astype(BF16)
    grad_low = cotangent.reshape(blk * seqs, width)
    grad_rows = grad_low.astype(F32)
    g_down = jnp.dot(acts_low.T, grad_low, preferred_element_type=F32).astype(BF16)
    s_down = reduce_rows(links, g_down)
    result = resid + jnp.dot(acts_low, mat_down, preferred_element_type=F32) + bias_down
    layer_output = result.astype(BF16).reshape(seqs, blk, width)
    g_down_bias = jnp.sum(grad_rows, axis=0)
    (d_upper,) = gelu_pull(jnp.dot(grad_low, mat_down.T, preferred_element_type=F32))
    d_upper_low = d_upper.astype(BF16)
    g_up = jnp.dot(normed2_low.T, d_upper_low, preferred_element_type=F32).astype(BF16)
    s_up = reduce_rows(links, g_up)
    g_up_bias = jnp.sum(d_upper_low.astype(F32), axis=0)
    d_resid, g_gain2, g_shift2 = ln2_pull(
        jnp.dot(d_upper_low, mat_up.T, preferred_element_type=F32)
    )
    d_resid = d_resid + grad_rows
    d_branch_low = d_resid.astype(BF16)
    g_out = jnp.dot(attn_low.T, d_branch_low, preferred_element_type=F32).astype(BF16)
    s_out = reduce_rows(links, g_out)
    g_out_bias = jnp.sum(d_branch_low.astype(F32), axis=0)
    d_attn_low = jnp.dot(d_branch_low, mat_out.T, preferred_element_type=F32).astype(BF16)
    d_attn4 = d_attn_low.reshape(blk, H, head_dim)
    delta = jnp.transpose(jnp.sum(d_attn4.astype(F32) * attention4, axis=-1), (1, 0))

    size = blk
    count = span // size

    def grad_step(dq_acc, block):
        piece_keys, piece_values, start = block
        dq, dk, dv = grad_block(
            queries4, d_attn4, piece_keys, piece_values, start, query_pos, lse, delta, scale
        )
        low = jnp.concatenate([dk.reshape(size, width), dv.reshape(size, width)], axis=1)
        return dq_acc + dq, low.astype(BF16)

    dq_acc, d_kv = lax.scan(
        grad_step,
        jnp.zeros((blk, H, head_dim), F32),
        (
            keys4.reshape(count, size, H, head_dim),
            values4.reshape(count, size, H, head_dim),
            jnp.arange(count, dtype=jnp.int32) * size,
        ),
    )
    d_kv = d_kv.reshape(span, 2 * width)
    d_queries_low = dq_acc.reshape(blk, width).astype(BF16)
    g_q = jnp.dot(normed1_low.T, d_queries_low, preferred_element_type=F32).astype(BF16)
    g_kv = jnp.dot(normed_all.T, d_kv, preferred_element_type=F32).astype(BF16)
    s_qkv = jnp.concatenate([reduce_rows(links, g_q), reduce_rows(links, g_kv)], axis=1)
    g_q_bias = jnp.sum(d_queries_low.astype(F32), axis=0)
    g_v_bias = jnp.sum(d_kv[:, width:].astype(F32), axis=0)

    d_blocks = jnp.dot(d_kv, mat_qkv[:, width:].T, preferred_element_type=F32).astype(BF16)
    part = d_blocks.reshape(links.high, 2, 2, blk, width)
    got = links.other_core(pick(part, 1 - links.core, 2))
    have = [pick(part, links.core, 2), got]
    sent = total([pick(item, 1 - links.row, 1) for item in have]).astype(BF16)
    have = [pick(item, links.row, 1) for item in have] + [links.other_row(sent)]
    levels = links.high
    for bit in reversed(range(2, links.nctx.bit_length() - 1)):
        levels //= 2
        mine = (links.ctx // (1 << bit)) % 2
        have = [item.reshape(2, levels, blk, width) for item in have]
        sent = total([pick(item, 1 - mine) for item in have]).astype(BF16)
        have = [pick(item, mine) for item in have] + [links.flip(sent, 1 << bit)]
    d_normed1 = total(have).reshape(blk, width) + jnp.dot(
        d_queries_low, mat_qkv[:, :width].T, preferred_element_type=F32
    )
    d_rows, g_gain1, g_shift1 = ln1_pull(d_normed1)
    input_grad = (d_rows + d_resid).astype(BF16).reshape(seqs, blk, width)

    flat = jnp.concatenate(
        [
            jnp.stack(
                [g_gain1, g_shift1, g_q_bias, g_v_bias, g_out_bias, g_gain2, g_shift2, g_down_bias]
            ).reshape(-1),
            g_up_bias,
        ]
    )
    flat = lax.psum(flat, ("dp", "ctx", "wshard"))
    names = []
    for index in range(8):
        names.append(lax.dynamic_slice_in_dim(flat, index * width + side * half, half, 0))
    s_up_bias = lax.dynamic_slice_in_dim(flat, 8 * width + side * (ff // 2), ff // 2, 0)
    s_gain1, s_shift1, s_q_bias, s_v_bias, s_out_bias, s_gain2, s_shift2, s_down_bias = names
    return (
        layer_output,
        input_grad,
        s_gain1,
        s_shift1,
        s_qkv,
        s_q_bias,
        s_v_bias,
        s_out,
        s_out_bias,
        s_gain2,
        s_shift2,
        s_up,
        s_up_bias,
        s_down,
        s_down_bias,
    )


def solution(mesh):
    sizes = dict(mesh.shape)

    def body(*args):
        return shards(sizes, *args)

    row = P(("dp", "wshard"), "ctx", None)
    vec, mat = P("wshard"), P("wshard", None)
    return jax.shard_map(
        body,
        mesh=mesh,
        in_specs=(row, vec, vec, mat, vec, vec, mat, vec, vec, vec, mat, vec, mat, vec, row),
        out_specs=(row, row, vec, vec, mat, vec, vec, mat, vec, vec, vec, mat, vec, mat, vec),
        check_vma=False,
    )
```

```python
import functools

import jax
import jax.numpy as jnp
from jax import lax
from jax.experimental import pallas as pl
from jax.experimental.pallas import tpu as pltpu
from jax.experimental.layout import Layout, with_layout_constraint
from jax.sharding import PartitionSpec as P


H = 17
F32 = jnp.float32
BF16 = jnp.bfloat16
GRID = ("dp", "ctx")

NT = (((1,), (1,)), ((), ()))
NN = (((1,), (0,)), ((), ()))


def layer_norm(values, gain, shift):
    mean = jnp.mean(values, axis=-1, keepdims=True)
    centred = values - mean
    variance = jnp.mean(centred * centred, axis=-1, keepdims=True)
    return centred * lax.rsqrt(variance + 1e-05) * gain + shift


def exact_gelu(values):
    return jax.nn.gelu(values, approximate=False)


def pick(array, index, axis=0):
    return lax.dynamic_index_in_dim(array, index, axis, keepdims=False)


def row_major(array):
    return with_layout_constraint(array, Layout(tuple(range(array.ndim))))


def ordered(first_mine, mine, other):
    return jnp.stack(
        [jnp.where(first_mine, mine, other), jnp.where(first_mine, other, mine)], axis=0
    )


class Links:
    def __init__(self, sizes):
        self.ndp, self.nctx, self.nw = sizes["dp"], sizes["ctx"], sizes["wshard"]
        self.high = self.nctx // 4
        self.rest = self.ndp * self.high
        ctx = lax.axis_index("ctx")
        self.ctx = ctx
        self.side = lax.axis_index("wshard")
        self.core = ctx % 2
        self.row = (ctx // 2) % 2
        self.place = lax.axis_index("dp") * self.high + ctx // 4

    def across(self, array):
        return lax.ppermute(array, "wshard", [(0, 1), (1, 0)])

    def flip(self, array, bit):
        return lax.ppermute(array, "ctx", [(i, i ^ bit) for i in range(self.nctx)])

    def other_core(self, array):
        return self.flip(array, 1)

    def other_row(self, array):
        return self.flip(array, 2)

    def moved(self, array, target_of):
        pairs = []
        for place in range(self.rest):
            for low in range(4):

                def flat(p):
                    return (p // self.high) * self.nctx + (p % self.high) * 4 + low

                pairs.append((flat(place), flat(target_of(place))))
        return lax.ppermute(array, GRID, pairs)

    def shifted(self, array, step):
        return self.moved(array, lambda p: (p + step) % self.rest)


def assemble(links, own):
    axis = own.ndim - 2
    rows = own.shape[axis]
    quarter = rows // 2
    piece = lax.dynamic_slice_in_dim(own, links.core * quarter, quarter, axis)
    mine = row_major(links.across(row_major(piece)))
    theirs = row_major(links.other_core(mine))
    full = row_major(jnp.concatenate([own, own], axis=axis))
    base = (1 - links.side) * rows
    full = lax.dynamic_update_slice_in_dim(full, mine, base + links.core * quarter, axis)
    full = lax.dynamic_update_slice_in_dim(full, theirs, base + (1 - links.core) * quarter, axis)
    return row_major(full)


def window(tiles, count):
    size = -(-tiles // count)
    while count > 1 and ((tiles - size) % (count - 1) != 0 or (tiles - size) // (count - 1) > size):
        size += 1
    return size, ((tiles - size) // (count - 1) if count > 1 else 0)


def total(pieces):
    result = pieces[0].astype(F32)
    for piece in pieces[1:]:
        result = result + piece.astype(F32)
    return result


def reduce_rows(links, grad, row_first=False):
    rows, cols = grad.shape
    tiles = rows // 64
    view = row_major(grad).reshape(2, 2, 2, tiles, 8, cols)

    def outgoing(items, index, axis):
        return row_major(total([pick(item, index, axis) for item in items]).astype(BF16))

    sent = row_major(pick(view, 1 - links.core, 1))
    have = [pick(view, links.core, 1), links.other_core(sent)]
    for along in ("row", "side") if row_first else ("side", "row"):
        if along == "side":
            sent = outgoing(have, 1 - links.side, 0)
            have = [pick(item, links.side, 0) for item in have]
            have.append(links.across(sent))
        else:
            axis = have[0].ndim - 4
            sent = outgoing(have, 1 - links.row, axis)
            have = [pick(item, links.row, axis) for item in have]
            have.append(links.other_row(sent))
    mixed = row_major(total(have).astype(BF16))
    size, step = window(tiles, links.rest)

    def slot(index):
        return row_major(
            lax.dynamic_slice_in_dim(mixed, (index % links.rest) * step, size, 0)
        )

    final = [slot(links.place)]
    for shift in range(1, links.rest):
        final.append(links.shifted(slot(links.place + shift), shift))
    done = row_major(total(final).astype(BF16))
    whole = lax.dynamic_update_slice_in_dim(mixed, done, links.place * step, 0)
    for shift in range(1, links.rest):
        came = (links.place - shift + links.rest) % links.rest
        whole = lax.dynamic_update_slice_in_dim(whole, links.shifted(done, shift), came * step, 0)
    whole = row_major(whole)
    both = row_major(ordered(links.row == 0, whole, links.other_row(whole)))
    full = ordered(links.core == 0, both, links.other_core(both))
    return full.reshape(rows // 2, cols).astype(F32)


def reduce_vectors(links, flat):
    flat = flat + links.other_core(flat)
    flat = flat + links.across(flat)
    flat = flat + links.other_row(flat)
    bit = 1
    while bit < links.rest:
        flat = flat + links.moved(flat, lambda p, b=bit: p ^ b)
        bit *= 2
    return flat


def gather_context(links, own):
    blocks = ordered(links.row == 0, own, links.other_row(own))[:, None]
    for bit in range(2, links.nctx.bit_length() - 1):
        low = (links.ctx // (1 << bit)) % 2 == 0
        blocks = ordered(low, blocks, links.flip(blocks, 1 << bit)).reshape(
            (-1,) + blocks.shape[1:]
        )
    blocks = row_major(blocks)
    got = links.other_core(blocks)
    first = jnp.where(links.core == 0, blocks, got)
    second = jnp.where(links.core == 0, got, blocks)
    return row_major(
        jnp.concatenate([first, second], axis=1).reshape((links.nctx,) + own.shape)
    )


def mm(a, b, dims):
    return lax.dot_general(a, b, dims, preferred_element_type=F32)


def lane_mask(head, rows):
    lanes = lax.broadcasted_iota(jnp.int32, (rows, 128), 1)
    return (lanes < 64) if head == 0 else (lanes >= 64)


def causal(rows):
    keys = lax.broadcasted_iota(jnp.int32, (rows, rows), 0)
    return keys <= lax.broadcasted_iota(jnp.int32, (rows, rows), 1)


def forward_kernel(heads, blk, here_ref, q_ref, k_ref, v_ref, out_ref, lse_ref):
    pair = pl.program_id(0)
    here = here_ref[0]
    wide = heads * 64
    inside = lax.broadcasted_iota(jnp.int32, (blk, 128), 1) + pair * 128 < wide

    def clean(x):
        return jnp.where(inside, x, jnp.zeros_like(x))

    query = clean(q_ref[...]) * jnp.asarray(0.125, BF16)
    zero = jnp.zeros_like(query)
    qs = [jnp.where(lane_mask(head, blk), query, zero) for head in range(2)]

    def step(start, carry, masked):
        keys = clean(k_ref[pl.ds(start, blk), :])
        vals_t = clean(v_ref[pl.ds(start, blk), :]).T
        scores = [mm(keys, qs[head], NT) for head in range(2)]
        if masked:
            keep = causal(blk)
            scores = [jnp.where(keep, item, -1e30) for item in scores]
        out = []
        for head in range(2):
            best, norm, acc = carry[head]
            top = jnp.maximum(best, jnp.max(scores[head], axis=0, keepdims=True))
            probs = jnp.exp(scores[head] - top)
            shrink = jnp.exp(best - top)
            norm = norm * shrink + jnp.sum(probs, axis=0, keepdims=True)
            vt = vals_t[64 * head : 64 * head + 64]
            acc = acc * shrink + mm(vt, probs.astype(BF16), NN)
            out.append((top, norm, acc))
        return tuple(out)

    first = (
        jnp.full((1, blk), -1e30, F32),
        jnp.zeros((1, blk), F32),
        jnp.zeros((64, blk), F32),
    )
    state = step(pl.multiple_of(here * blk, blk), (first, first), True)
    state = lax.fori_loop(
        0, here, lambda j, c: step(pl.multiple_of(j * blk, blk), c, False), state
    )
    results = []
    for head in range(2):
        best, norm, acc = state[head]
        results.append(acc / norm)
        lse_ref[0, head : head + 1, :] = best + jnp.log(norm)
    out_ref[...] = jnp.concatenate(results, axis=0).T.astype(BF16)


def backward_kernel(
    heads, blk, span, first, here_ref, q_ref, k_ref, v_ref, o_ref, g_ref, lse_ref, dq_ref, dk_ref, dv_ref
):
    pair = pl.program_id(0) + first
    here = here_ref[0]
    wide = heads * 64
    inside = lax.broadcasted_iota(jnp.int32, (blk, 128), 1) + pair * 128 < wide

    def clean(x):
        return jnp.where(inside, x, jnp.zeros_like(x))

    query = clean(q_ref[...]) * jnp.asarray(0.125, BF16)
    dout = clean(g_ref[...])
    prod = (dout.astype(F32) * clean(o_ref[...]).astype(F32)).T
    deltas = [jnp.sum(prod[:64], axis=0, keepdims=True), jnp.sum(prod[64:], axis=0, keepdims=True)]
    zero = jnp.zeros_like(query)
    qs = [jnp.where(lane_mask(head, blk), query, zero) for head in range(2)]
    gs = [jnp.where(lane_mask(head, blk), dout, zero) for head in range(2)]

    def step(start, dq, masked):
        keys = clean(k_ref[pl.ds(start, blk), :])
        vals = clean(v_ref[pl.ds(start, blk), :])
        keys_t = keys.T
        dk = jnp.zeros((blk, 128), F32)
        dv = jnp.zeros((blk, 128), F32)
        dqs = []
        for head in range(2):
            scores = mm(keys, qs[head], NT)
            probs = jnp.exp(scores - lse_ref[0, head : head + 1, :])
            if masked:
                probs = jnp.where(causal(blk), probs, 0.0)
            dprobs = mm(vals, gs[head], NT)
            dscores = (probs * (dprobs - deltas[head])).astype(BF16)
            dv = dv + mm(probs.astype(BF16), gs[head], NN)
            dk = dk + mm(dscores, qs[head], NN)
            dqs.append(mm(keys_t[64 * head : 64 * head + 64], dscores, NN))
        dk_ref[pl.ds(start, blk), :] = dk.astype(BF16)
        dv_ref[pl.ds(start, blk), :] = dv.astype(BF16)
        return dq + jnp.concatenate(dqs, axis=0)

    dq = step(pl.multiple_of(here * blk, blk), jnp.zeros((128, blk), F32), True)
    dq = lax.fori_loop(0, here, lambda j, c: step(pl.multiple_of(j * blk, blk), c, False), dq)
    dq_ref[...] = (dq * 0.125).T.astype(BF16)

    def blank(j, carry):
        start = pl.multiple_of(j * blk, blk)
        dk_ref[pl.ds(start, blk), :] = jnp.zeros((blk, 128), BF16)
        dv_ref[pl.ds(start, blk), :] = jnp.zeros((blk, 128), BF16)
        return carry

    lax.fori_loop(here + 1, span // blk, blank, 0)


def attention_forward(here, queries, keys, values, heads):
    blk, width = queries.shape
    span = keys.shape[0]
    pairs = (heads + 1) // 2
    block = pl.BlockSpec((blk, 128), lambda p, h: (0, p))
    whole = pl.BlockSpec((span, 128), lambda p, h: (0, p))
    flops = 4 * blk * span * 128 * 2 * pairs
    return pl.pallas_call(
        functools.partial(forward_kernel, heads, blk),
        grid_spec=pltpu.PrefetchScalarGridSpec(
            num_scalar_prefetch=1,
            grid=(pairs,),
            in_specs=[block, whole, whole],
            out_specs=[block, pl.BlockSpec((1, 2, blk), lambda p, h: (p, 0, 0))],
        ),
        out_shape=[
            jax.ShapeDtypeStruct((blk, width), BF16),
            jax.ShapeDtypeStruct((pairs, 2, blk), F32),
        ],
        cost_estimate=pl.CostEstimate(
            flops=flops, bytes_accessed=4 * span * width, transcendentals=blk * span * heads
        ),
        name="attention_forward",
    )(here, queries, keys, values)


def attention_backward(here, queries, keys, values, attention, douts, lse, heads, first, count):
    blk, _ = queries.shape
    span = keys.shape[0]
    block = pl.BlockSpec((blk, 128), lambda p, h: (0, p + first))
    whole = pl.BlockSpec((span, 128), lambda p, h: (0, p + first))
    block_out = pl.BlockSpec((blk, 128), lambda p, h: (0, p))
    whole_out = pl.BlockSpec((span, 128), lambda p, h: (0, p))
    return pl.pallas_call(
        functools.partial(backward_kernel, heads, blk, span, first),
        grid_spec=pltpu.PrefetchScalarGridSpec(
            num_scalar_prefetch=1,
            grid=(count,),
            in_specs=[
                block,
                whole,
                whole,
                block,
                block,
                pl.BlockSpec((1, 2, blk), lambda p, h: (p + first, 0, 0)),
            ],
            out_specs=[block_out, whole_out, whole_out],
        ),
        out_shape=[
            jax.ShapeDtypeStruct((blk, 128 * count), BF16),
            jax.ShapeDtypeStruct((span, 128 * count), BF16),
            jax.ShapeDtypeStruct((span, 128 * count), BF16),
        ],
        cost_estimate=pl.CostEstimate(
            flops=20 * blk * span * 128 * count,
            bytes_accessed=8 * span * 128 * count,
            transcendentals=2 * blk * span * count,
        ),
    )(here, queries, keys, values, attention, douts, lse)


def shards(
    sizes,
    layer_input,
    ln1_gain,
    ln1_bias,
    w_qkv,
    q_bias,
    v_bias,
    w_out,
    out_bias,
    ln2_gain,
    ln2_bias,
    w_up,
    up_bias,
    w_down,
    down_bias,
    cotangent,
):
    links = Links(sizes)
    seqs, blk, width = layer_input.shape
    half = width // 2
    ff = up_bias.shape[0] * 2
    side = links.side

    small = [ln1_gain, ln1_bias, q_bias, v_bias, out_bias, ln2_gain, ln2_bias, down_bias]
    packed = jnp.stack(small, axis=0)
    packed_other = links.across(packed)
    vectors = jnp.where(
        side == 0,
        jnp.concatenate([packed, packed_other], axis=1),
        jnp.concatenate([packed_other, packed], axis=1),
    ).astype(F32)
    gain1, shift1, bias_q, bias_v, bias_out, gain2, shift2, bias_down = (
        vectors[i] for i in range(8)
    )
    bias_up = ordered(side == 0, up_bias, links.across(up_bias))
    bias_up = bias_up.reshape(ff).astype(F32)

    packed_qkv = jnp.stack([w_qkv[:, i * width : (i + 1) * width] for i in range(3)])
    mat_q, mat_k, mat_v = assemble(links, packed_qkv)
    mat_out = assemble(links, w_out)
    mat_up = assemble(links, w_up)
    mat_down = assemble(links, w_down)

    span = seqs * links.nctx * blk
    every = gather_context(links, layer_input.reshape(seqs * blk, width)).reshape(span, width)
    rows = layer_input.reshape(seqs * blk, width).astype(F32)
    normed1, ln1_pull = jax.vjp(layer_norm, rows, gain1, shift1)
    normed1_low = row_major(normed1.astype(BF16))
    normed_all = row_major(layer_norm(every.astype(F32), gain1, shift1).astype(BF16))
    queries = (jnp.dot(normed1_low, mat_q, preferred_element_type=F32) + bias_q).astype(BF16)
    keys = jnp.dot(normed_all, mat_k, preferred_element_type=F32).astype(BF16)
    values = (jnp.dot(normed_all, mat_v, preferred_element_type=F32) + bias_v).astype(BF16)
    place = links.ctx.astype(jnp.int32)[None]
    attn_low, lse = attention_forward(place, queries, keys, values, H)
    resid = rows + jnp.dot(attn_low, mat_out, preferred_element_type=F32) + bias_out
    normed2, ln2_pull = jax.vjp(layer_norm, resid, gain2, shift2)
    normed2_low = row_major(normed2.astype(BF16))
    upper = jnp.dot(normed2_low, mat_up, preferred_element_type=F32) + bias_up
    acts, gelu_pull = jax.vjp(exact_gelu, upper)
    acts_low = row_major(acts.astype(BF16))
    grad_low = cotangent.reshape(blk * seqs, width)
    grad_rows = grad_low.astype(F32)
    g_down = jnp.dot(acts_low.T, grad_low, preferred_element_type=F32).astype(BF16)
    s_down = reduce_rows(links, g_down)
    (d_upper,) = gelu_pull(jnp.dot(grad_low, mat_down.T, preferred_element_type=F32))
    d_upper_low = row_major(d_upper.astype(BF16))
    g_up = jnp.dot(normed2_low.T, d_upper_low, preferred_element_type=F32).astype(BF16)
    s_up = reduce_rows(links, g_up, True)
    d_normed2 = jnp.dot(d_upper_low, mat_up.T, preferred_element_type=F32)
    d_resid, g_gain2, g_shift2 = ln2_pull(d_normed2)
    d_resid = d_resid + grad_rows
    d_branch_low = row_major(d_resid.astype(BF16))
    g_out = jnp.dot(attn_low.T, d_branch_low, preferred_element_type=F32).astype(BF16)
    s_out = reduce_rows(links, g_out, True)
    d_attn_low = jnp.dot(d_branch_low, mat_out.T, preferred_element_type=F32).astype(BF16)
    result = resid + jnp.dot(acts_low, mat_down, preferred_element_type=F32) + bias_down
    layer_output = result.astype(BF16).reshape(seqs, blk, width)
    groups = []
    for part in range(3):
        groups.append(
            attention_backward(
                place, queries, keys, values, attn_low, d_attn_low, lse, H, 3 * part, 3
            )
        )
    pieces = []
    for part, (dq, dk, dv) in enumerate(groups):
        g_part = jnp.concatenate(
            [
                jnp.dot(normed1_low.T, dq, preferred_element_type=F32).astype(BF16),
                jnp.dot(normed_all.T, dk, preferred_element_type=F32).astype(BF16),
                jnp.dot(normed_all.T, dv, preferred_element_type=F32).astype(BF16),
            ],
            axis=1,
        )
        pieces.append(reduce_rows(links, g_part, part == 1))
    last = width - 768
    s_qkv = jnp.concatenate(
        [
            pieces[part][:, 384 * which : 384 * which + (last if part == 2 else 384)]
            for which in range(3)
            for part in range(3)
        ],
        axis=1,
    )
    d_queries_low, d_keys, d_values = (
        jnp.concatenate([group[which] for group in groups], axis=1)[:, :width]
        for which in range(3)
    )
    g_down_bias = jnp.sum(grad_rows, axis=0)
    g_up_bias = jnp.sum(d_upper_low.astype(F32), axis=0)
    g_out_bias = jnp.sum(d_branch_low.astype(F32), axis=0)
    g_q_bias = jnp.sum(d_queries_low.astype(F32), axis=0)
    g_v_bias = jnp.sum(d_values.astype(F32), axis=0)

    d_blocks = (
        jnp.dot(d_keys, mat_k.T, preferred_element_type=F32)
        + jnp.dot(d_values, mat_v.T, preferred_element_type=F32)
    ).astype(BF16)
    part = d_blocks.reshape(links.high, 2, 2, blk, width)
    got = links.other_core(pick(part, 1 - links.core, 2))
    have = [pick(part, links.core, 2), got]
    sent = total([pick(item, 1 - links.row, 1) for item in have]).astype(BF16)
    have = [pick(item, links.row, 1) for item in have] + [links.other_row(sent)]
    levels = links.high
    for bit in reversed(range(2, links.nctx.bit_length() - 1)):
        levels //= 2
        mine = (links.ctx // (1 << bit)) % 2
        have = [item.reshape(2, levels, blk, width) for item in have]
        sent = total([pick(item, 1 - mine) for item in have]).astype(BF16)
        have = [pick(item, mine) for item in have] + [links.flip(sent, 1 << bit)]
    d_normed1 = total(have).reshape(blk, width) + jnp.dot(
        d_queries_low, mat_q.T, preferred_element_type=F32
    )
    d_rows, g_gain1, g_shift1 = ln1_pull(d_normed1)
    input_grad = (d_rows + d_resid).astype(BF16).reshape(seqs, blk, width)

    flat = jnp.concatenate(
        [
            jnp.stack(
                [g_gain1, g_shift1, g_q_bias, g_v_bias, g_out_bias, g_gain2, g_shift2, g_down_bias]
            ).reshape(-1),
            g_up_bias,
        ]
    )
    flat = reduce_vectors(links, flat)
    names = []
    for index in range(8):
        names.append(lax.dynamic_slice_in_dim(flat, index * width + side * half, half, 0))
    s_up_bias = lax.dynamic_slice_in_dim(flat, 8 * width + side * (ff // 2), ff // 2, 0)
    s_gain1, s_shift1, s_q_bias, s_v_bias, s_out_bias, s_gain2, s_shift2, s_down_bias = names
    return (
        layer_output,
        input_grad,
        s_gain1,
        s_shift1,
        s_qkv,
        s_q_bias,
        s_v_bias,
        s_out,
        s_out_bias,
        s_gain2,
        s_shift2,
        s_up,
        s_up_bias,
        s_down,
        s_down_bias,
    )


def solution(mesh):
    sizes = dict(mesh.shape)

    def body(*args):
        return shards(sizes, *args)

    row = P(("dp", "wshard"), "ctx", None)
    vec, mat = P("wshard"), P("wshard", None)
    return jax.shard_map(
        body,
        mesh=mesh,
        in_specs=(row, vec, vec, mat, vec, vec, mat, vec, vec, vec, mat, vec, mat, vec, row),
        out_specs=(row, row, vec, vec, mat, vec, vec, mat, vec, vec, vec, mat, vec, mat, vec),
        check_vma=False,
    )
```
